32 devices in a mesh: wide: 16 (over z, y, x), narrow: 2 (over core).
Axes of the slice: x: 2, y: 2, z: 4, core: 2. Of those that a mesh axis runs over, the one named last changes fastest.
Arguments:
- node_latent: bfloat16 [4096, 512], P(('wide', 'narrow')), may hold values from -6 to 6
- edge_latent: bfloat16 [16384, 512], P(('wide', 'narrow')), may hold values from -6 to 6
- node_cotangent: bfloat16 [4096, 512], P(('wide', 'narrow')), may hold values from -6 to 6
- w_first: bfloat16 [1536, 512], replicated, may hold values from -2 to 2
- bias_first: bfloat16 [512], replicated, may hold values from -4 to 4
- w_second: bfloat16 [512, 512], replicated, may hold values from -2 to 2
- bias_second: bfloat16 [512], replicated, may hold values from -4 to 4
- norm_gain: bfloat16 [512], replicated, may hold values from 0.099609375 to 1.8984375
- send_map: int32 [32, 4, 64], P(('wide', 'narrow')), may hold values from -1 to 127, as said below
- edge_sender: int32 [16384], P(('wide', 'narrow')), may hold values from 0 to 383, as said below
- edge_receiver: int32 [16384], P(('wide', 'narrow')), may hold values from 0 to 127
Outputs:
- node_grad: bfloat16 [4096, 512], P(('wide', 'narrow'))
- edge_grad: bfloat16 [16384, 512], P(('wide', 'narrow'))
- first_update: float32 [1536, 512], P('wide')
- second_update: float32 [512, 512], P('wide')
The draws below stay inside these ranges and needn't reach their ends.
Inputs may be any that keep to these rules, and one draw needn't show every extreme that they name: `send_map`: -1 marks an unused slot; in each row the used slots come first, at most 64, about a third of them on average; in every draw some partition uses all 64 slots toward a wide neighbour; partitions at narrow index 0 send nothing toward block 3 of a lower neighbour and those at the last narrow index nothing toward a higher one. `edge_sender`: a value below 128 is a local node; 128 + k * 64 + s names slot s of received block k, and only slots that the sending partition uses are named.
All inputs are finite; a program needn't handle non-finite values.
Results may differ from the reference program's by a relative error of at most 0.0085.
Values may be sent and summed in bfloat16 or wider, within the bound.
No kernel may reach another device: no remote copies, remote signals or barrier semaphores. Data moves between devices by JAX's collectives and lax.ppermute only.
A program may use at most 64 MiB of HBM per device.

```python
import math
import jax
import jax.numpy as jnp
from jax import lax

D = 512
NODE_DEV = 128
EDGE_DEV = 512
HALO = 64
NODES = 4096
EDGES = 16384
N_WIDE = 16
N_NARROW = 2
DEVICES = 32


def halo_counts(key):
    base_key = jax.random.fold_in(key, 101)
    counts = jax.random.randint(jax.random.fold_in(base_key, 1), (DEVICES, 4), 1, 2 * HALO // 3 + 1)
    full_device = jax.random.randint(jax.random.fold_in(base_key, 2), (), 0, DEVICES)
    full_direction = jax.random.randint(jax.random.fold_in(base_key, 3), (), 0, 2)
    row_ids = jnp.arange(DEVICES, dtype=jnp.int32)[:, None]
    col_ids = jnp.arange(4, dtype=jnp.int32)[None, :]
    counts = jnp.where((row_ids == full_device) & (col_ids == full_direction), HALO, counts)
    narrow_index = row_ids % N_NARROW
    counts = jnp.where((col_ids == 2) & (narrow_index == N_NARROW - 1), 0, counts)
    counts = jnp.where((col_ids == 3) & (narrow_index == 0), 0, counts)
    return counts.astype(jnp.int32)


def draw_send_map(key, part):
    counts = halo_counts(key)
    chosen = jax.random.randint(jax.random.fold_in(key, 102), (DEVICES, 4, HALO), 0, NODE_DEV)
    slot_index = jnp.arange(HALO, dtype=jnp.int32)
    return jnp.where(slot_index[None, None, :] < counts[:, :, None], chosen, -1).astype(jnp.int32)


def draw_edge_sender(key, part):
    counts = halo_counts(key).reshape(N_WIDE, N_NARROW, 4)
    zero_col = jnp.zeros_like(counts[:, :1, 0])
    from_lower = jnp.roll(counts[:, :, 0], 1, axis=0)
    from_higher = jnp.roll(counts[:, :, 1], -1, axis=0)
    from_below = jnp.concatenate([zero_col, counts[:, :-1, 2]], 1)
    from_above = jnp.concatenate([counts[:, 1:, 3], zero_col], 1)
    incoming = jnp.stack([from_lower, from_higher, from_below, from_above], -1).reshape(DEVICES, 4)
    device = jnp.arange(EDGES, dtype=jnp.int32) // EDGE_DEV
    kind_draw = jax.random.randint(jax.random.fold_in(key, 103), (EDGES,), 0, 10)
    direction = jax.random.randint(jax.random.fold_in(key, 104), (EDGES,), 0, 4)
    raw_slot = jax.random.randint(jax.random.fold_in(key, 105), (EDGES,), 0, 1 << 20)
    local_ids = jax.random.randint(jax.random.fold_in(key, 106), (EDGES,), 0, NODE_DEV)
    live_count = incoming[device, direction]
    remote = NODE_DEV + direction * HALO + raw_slot % jnp.maximum(live_count, 1)
    use_remote = (kind_draw < 4) & (live_count > 0)
    return jnp.where(use_remote, remote, local_ids).astype(jnp.int32)


def scaled_weight(key, row_count, col_count):
    base_draw = jnp.clip(jax.random.normal(jax.random.fold_in(key, 1), (row_count, col_count), jnp.float32), -3.0, 3.0)
    row_scale = jnp.exp(jax.random.uniform(jax.random.fold_in(key, 2), (row_count, 1), jnp.float32, math.log(0.3), math.log(3.0)))
    col_scale = jnp.exp(jax.random.uniform(jax.random.fold_in(key, 3), (1, col_count), jnp.float32, math.log(0.3), math.log(3.0)))
    return (base_draw * row_scale * col_scale / (1.39 * math.sqrt(row_count))).astype(jnp.bfloat16)


def draw_w_first(key, part):
    return scaled_weight(jax.random.fold_in(key, 21), 3 * D, D)


def draw_w_second(key, part):
    return scaled_weight(jax.random.fold_in(key, 22), D, D)


def place_ends(array, stream_key, low, top_value):
    longest = array.shape.index(max(array.shape))
    spots = []
    for shift in (0, 1):
        where = [jax.random.randint(jax.random.fold_in(stream_key, axis), (), 0, length) for axis, length in enumerate(array.shape)]
        where[longest] = (where[longest] + shift) % array.shape[longest]
        spots.append(tuple(where))
    return array.at[spots[0]].set(low).at[spots[1]].set(top_value)


def steps_of(own_key, extent, shards, low, top_value):
    loudness, own = 1.0, jax.random.fold_in(own_key, 6)
    for position, parts in shards:
        heights = jnp.exp(jax.random.uniform(jax.random.fold_in(own, position), (parts,), jnp.float32, low / len(shards), top_value / len(shards)))
        loudness = loudness * jnp.repeat(heights, extent[position] // parts).reshape([-1 if axis == position else 1 for axis in range(len(extent))])
    return loudness


def normal_values(stream_key, shape, spread, bound, cuts=(), kind=jnp.bfloat16):
    entries = spread * jax.random.normal(stream_key, shape, jnp.float32)
    if cuts:
        entries = entries * steps_of(stream_key, shape, cuts, -0.22, 0.18)
    return jnp.clip(entries, -bound, bound).astype(kind)


def setup_inputs(seed: int = 0) -> dict:
    key_of = jax.random.split(jax.random.key(seed), 12)
    node_latent = normal_values(key_of[0], (NODES, D), 1.0, 6.0, ((0, 32),))
    edge_latent = normal_values(key_of[1], (EDGES, D), 1.0, 6.0, ((0, 32),))
    node_cotangent = normal_values(key_of[2], (NODES, D), 1.0, 6.0, ((0, 32),))
    w_first = draw_w_first(jax.random.fold_in(key_of[11], 71), 0)
    bias_first = normal_values(key_of[4], (D,), 1.0, 4.0)
    w_second = draw_w_second(jax.random.fold_in(key_of[11], 71), 0)
    bias_second = normal_values(key_of[6], (D,), 1.0, 4.0)
    norm_gain = jnp.clip(1.0 + 0.18 * jax.random.normal(key_of[7], (D,), jnp.float32), 0.099609375, 1.8984375).astype(jnp.bfloat16)
    send_map = draw_send_map(jax.random.fold_in(key_of[11], 71), 0)
    edge_sender = draw_edge_sender(jax.random.fold_in(key_of[11], 71), 0)
    edge_receiver = place_ends(jax.random.randint(key_of[10], (EDGES,), 0, NODE_DEV), jax.random.fold_in(key_of[10], 1), 0, NODE_DEV - 1).astype(jnp.int32)
    return dict(node_latent=node_latent, edge_latent=edge_latent, node_cotangent=node_cotangent, w_first=w_first, bias_first=bias_first, w_second=w_second, bias_second=bias_second, norm_gain=norm_gain, send_map=send_map, edge_sender=edge_sender, edge_receiver=edge_receiver)


def narrow_shift(blocks, direction):
    zero_col = jnp.zeros_like(blocks[:, :1])
    if direction == 1:
        return jnp.concatenate([zero_col, blocks[:, :-1]], 1)
    return jnp.concatenate([blocks[:, 1:], zero_col], 1)

def norm_parts(second_pre):
    mean_value = lax.optimization_barrier(jnp.mean(second_pre, -1, keepdims=True))
    centered = second_pre - mean_value
    variance = lax.optimization_barrier(jnp.mean(centered * centered, -1, keepdims=True))
    inv_std = lax.rsqrt(variance + 1e-05)
    return (centered * inv_std, inv_std)

def edge_terms(node_table, own_nodes, own_cot, own_edges, sender_ids, receiver_ids, w_first, bias_first, w_second, bias_second, norm_gain):
    feature_width = own_edges.shape[1]
    sender_rows = node_table[sender_ids]
    receiver_rows = own_nodes[receiver_ids]
    inputs = jnp.concatenate([own_edges, sender_rows, receiver_rows], 1)
    preact = jnp.dot(inputs, w_first, preferred_element_type=jnp.float32) + bias_first.astype(jnp.float32)
    activation = jax.nn.silu(preact).astype(jnp.bfloat16)
    second_pre = jnp.dot(activation, w_second, preferred_element_type=jnp.float32) + bias_second.astype(jnp.float32)
    normalized, inv_std = norm_parts(second_pre)
    upstream = own_cot[receiver_ids].astype(jnp.float32)
    scaled = upstream * norm_gain.astype(jnp.float32)
    norm_back = (inv_std * (scaled - lax.optimization_barrier(jnp.mean(scaled, -1, keepdims=True)) - normalized * lax.optimization_barrier(jnp.mean(scaled * normalized, -1, keepdims=True)))).astype(jnp.bfloat16)
    second_grad = jnp.dot(activation.T, norm_back, preferred_element_type=jnp.float32)
    sigmoid_pre = jax.nn.sigmoid(preact)
    pre_back = (jnp.dot(norm_back, w_second.T, preferred_element_type=jnp.float32) * sigmoid_pre * (1.0 + preact * (1.0 - sigmoid_pre))).astype(jnp.bfloat16)
    first_grad = jnp.dot(inputs.T, pre_back, preferred_element_type=jnp.float32)
    input_back = jnp.dot(pre_back, w_first.T, preferred_element_type=jnp.float32)
    edge_grad = (upstream + input_back[:, :feature_width]).astype(jnp.bfloat16)
    table_grad = jax.ops.segment_sum(input_back[:, feature_width:2 * feature_width], sender_ids, num_segments=node_table.shape[0])
    receiver_grad = jax.ops.segment_sum(input_back[:, 2 * feature_width:], receiver_ids, num_segments=own_nodes.shape[0])
    return (edge_grad, table_grad, receiver_grad, first_grad, second_grad)

def clip_update(grad_total, weight):
    row_count = grad_total.shape[0]
    grad_sq = lax.optimization_barrier(jnp.sum(grad_total * grad_total, 0))
    weight_sq = lax.optimization_barrier(jnp.sum(jnp.square(weight.astype(jnp.float32)), 0))
    unit_ratio = jnp.sqrt((grad_sq + 1e-06) / (weight_sq + 1e-06))
    mean_ratio = jnp.mean(unit_ratio)
    factor = jnp.minimum(1.0 / (mean_ratio * jnp.sqrt(weight_sq + 1e-06)), 1.0 / jnp.sqrt(grad_sq + 1e-06))
    return grad_total * factor * math.sqrt(row_count)

def reference(node_latent, edge_latent, node_cotangent, w_first, bias_first, w_second, bias_second, norm_gain, send_map, edge_sender, edge_receiver):
    node_blocks = node_latent.reshape(N_WIDE, N_NARROW, NODE_DEV, D)
    slot_map = send_map.reshape(N_WIDE, N_NARROW, 4, HALO)
    live_slot = slot_map >= 0
    safe_map = jnp.where(live_slot, slot_map, 0).astype(jnp.int32)
    wide_ids = jnp.arange(N_WIDE, dtype=jnp.int32)[:, None, None, None]
    narrow_ids = jnp.arange(N_NARROW, dtype=jnp.int32)[None, :, None, None]
    outgoing = node_blocks[wide_ids, narrow_ids, safe_map]
    outgoing = jnp.where(live_slot[..., None], outgoing, jnp.zeros_like(outgoing))
    received = jnp.stack([jnp.roll(outgoing[:, :, 0], 1, axis=0), jnp.roll(outgoing[:, :, 1], -1, axis=0), narrow_shift(outgoing[:, :, 2], 1), narrow_shift(outgoing[:, :, 3], -1)], 2)
    node_table = jnp.concatenate([node_blocks, received.reshape(N_WIDE, N_NARROW, 4 * HALO, D)], 2)
    cot_blocks = node_cotangent.reshape(N_WIDE, N_NARROW, NODE_DEV, D)
    edge_blocks = edge_latent.reshape(N_WIDE, N_NARROW, EDGE_DEV, D)
    sender_blocks = edge_sender.reshape(N_WIDE, N_NARROW, EDGE_DEV)
    receiver_blocks = edge_receiver.reshape(N_WIDE, N_NARROW, EDGE_DEV)

    def device_terms(table_part, node_part, cot_part, edge_part, sender_part, receiver_part):
        return edge_terms(table_part, node_part, cot_part, edge_part, sender_part, receiver_part, w_first, bias_first, w_second, bias_second, norm_gain)

    def edge_block(totals, block_data):
        edge_grad, table_grad, receiver_grad, first_grad, second_grad = jax.vmap(device_terms)(*block_data)
        totals = (totals[0] + lax.optimization_barrier(jnp.sum(first_grad, 0)), totals[1] + lax.optimization_barrier(jnp.sum(second_grad, 0)))
        return (totals, (edge_grad, table_grad, receiver_grad))
    initial = (jnp.zeros((3 * D, D), jnp.float32), jnp.zeros((D, D), jnp.float32))
    totals, outputs = lax.scan(edge_block, initial, (node_table, node_blocks, cot_blocks, edge_blocks, sender_blocks, receiver_blocks))
    edge_grads, table_grads, receiver_grads = outputs
    halo_grad = table_grads[:, :, NODE_DEV:].reshape(N_WIDE, N_NARROW, 4, HALO, D).astype(jnp.bfloat16)
    returned = jnp.stack([jnp.roll(halo_grad[:, :, 0], -1, axis=0), jnp.roll(halo_grad[:, :, 1], 1, axis=0), narrow_shift(halo_grad[:, :, 2], -1), narrow_shift(halo_grad[:, :, 3], 1)], 2)
    send_hot = (slot_map[..., None] == jnp.arange(NODE_DEV, dtype=jnp.int32)).astype(jnp.float32)
    back = jnp.einsum('abkhn,abkhd->abnd', send_hot, returned.astype(jnp.float32), precision=lax.Precision.HIGHEST)
    node_grad = (cot_blocks.astype(jnp.float32) + table_grads[:, :, :NODE_DEV] + receiver_grads + back).astype(jnp.bfloat16)
    first_update = clip_update(totals[0], w_first)
    second_update = clip_update(totals[1], w_second)
    return (node_grad.reshape(NODES, D), edge_grads.reshape(EDGES, D), first_update, second_update)
```

```python
import math

import jax
import jax.numpy as jnp
from jax import lax
from jax.sharding import PartitionSpec as P

BF = jnp.bfloat16
F32 = jnp.float32


def halo_routes(axis, base, ring):
    count = lax.axis_size(axis)
    if count % 2:
        up = [(i, (i + 1) % count) for i in range(count) if ring or i + 1 < count]
        return [(up, base, base), ([(t, s) for s, t in up], base + 1, base + 1)]
    odd = lax.axis_index(axis) % 2
    near = [(i, i ^ 1) for i in range(count)]
    far = [(i, ((i + 1) ^ 1) - 1) for i in range(count)]
    far = [(s, t % count) for s, t in far if ring or 0 <= t < count]
    routes = [(near, base + odd, base + 1 - odd)]
    if far:
        routes.insert(0, (far, base + 1 - odd, base + odd))
    return routes


def norm_parts(second_pre):
    mean_value = jnp.mean(second_pre, -1, keepdims=True)
    centered = second_pre - mean_value
    variance = jnp.mean(centered * centered, -1, keepdims=True)
    inv_std = lax.rsqrt(variance + 1e-05)
    return (centered * inv_std, inv_std)


def clip_share(grad_share, grad_sq, weight_sq, fan_rows):
    unit_ratio = jnp.sqrt((grad_sq + 1e-06) / (weight_sq + 1e-06))
    mean_ratio = jnp.mean(unit_ratio)
    factor = jnp.minimum(
        1.0 / (mean_ratio * jnp.sqrt(weight_sq + 1e-06)), 1.0 / jnp.sqrt(grad_sq + 1e-06)
    )
    return grad_share * (factor * math.sqrt(fan_rows))


def contract(hot, values):
    high = values.astype(BF)
    low = (values - high.astype(F32)).astype(BF)
    dims = (((0,), (0,)), ((), ()))
    return lax.dot_general(hot, high, dims, preferred_element_type=F32) + lax.dot_general(
        hot, low, dims, preferred_element_type=F32
    )


def swap_pairs(size, mask):
    return [(i, i ^ mask) for i in range(size)]


def pick(value, axis, index):
    return lax.dynamic_index_in_dim(value, index, axis, keepdims=False)


def reduce_weights(first_grad, second_grad):
    wide, narrow = lax.axis_size("wide"), lax.axis_size("narrow")
    a, b = lax.axis_index("wide"), lax.axis_index("narrow")
    width = first_grad.shape[1]
    first_rows, second_rows = first_grad.shape[0] // wide, second_grad.shape[0] // wide
    rows = first_rows + second_rows
    value = jnp.concatenate(
        [
            first_grad.reshape(wide, first_rows, width),
            second_grad.reshape(wide, second_rows, width),
        ],
        1,
    )
    span, mask = width, narrow // 2
    while mask:
        span //= 2
        bit = (b // mask) % 2
        sent = lax.dynamic_slice_in_dim(value, (1 - bit) * span, span, 2).astype(BF)
        kept = lax.dynamic_slice_in_dim(value, bit * span, span, 2)
        value = kept + lax.ppermute(sent, "narrow", swap_pairs(narrow, mask)).astype(F32)
        mask //= 2
    bits = wide.bit_length() - 1
    low, high = a % 2, (a // 2) % 2
    flip = b % 2
    value = value.reshape(wide // 4, 2, 2, rows, span)
    both = ("wide", "narrow")

    def crossed(value, even_mask, odd_mask):
        pairs = []
        for i in range(wide):
            for j in range(narrow):
                pairs.append((i * narrow + j, (i ^ (odd_mask if j % 2 else even_mask)) * narrow + j))
        return lax.ppermute(value.astype(BF), both, pairs).astype(F32)

    sent = jnp.where(flip == 0, pick(value, 2, 1 - low), pick(value, 1, 1 - high))
    kept = jnp.where(flip == 0, pick(value, 2, low), pick(value, 1, high))
    value = kept + crossed(sent, 1, 2)
    left = jnp.where(flip == 0, high, low)
    value = pick(value, 1, left) + crossed(pick(value, 1, 1 - left), 2, 1)
    for position in range(2, bits - 1):
        value = value.reshape(value.shape[0] // 2, 2, rows, span)
        bit = (a >> position) % 2
        value = pick(value, 1, bit) + crossed(pick(value, 1, 1 - bit), 1 << position, 1 << position)
    top = wide // 2
    value = value.reshape(2, rows, span)
    value = value + crossed(value, top, top)
    mask = 1
    while mask < narrow:
        other = lax.ppermute(value, "narrow", swap_pairs(narrow, mask))
        bit = (b // mask) % 2
        value = jnp.where(
            bit == 0,
            jnp.concatenate([value, other], 2),
            jnp.concatenate([other, value], 2),
        )
        mask *= 2
    squares = value * value
    sums = jnp.stack([squares[:, :first_rows].sum((0, 1)), squares[:, first_rows:].sum((0, 1))], 0)
    for position in range(bits - 1):
        sums = sums + lax.ppermute(sums, "wide", swap_pairs(wide, 1 << position))
    share = pick(value, 0, a // top)
    return share[:first_rows], share[first_rows:], sums[0], sums[1]


def per_device(
    node_latent,
    edge_latent,
    node_cotangent,
    w_first,
    bias_first,
    w_second,
    bias_second,
    norm_gain,
    send_map,
    edge_sender,
    edge_receiver,
):
    node_count, feature_width = node_latent.shape
    halo_slots = send_map.shape[2]
    routes = [("wide", r) for r in halo_routes("wide", 0, True)]
    routes += [("narrow", r) for r in halo_routes("narrow", 2, False)]
    blocks = len(routes)
    table_rows = node_count + blocks * halo_slots
    sent_slots = jnp.stack([pick(send_map[0], 0, sent) for _, (_, sent, _) in routes], 0)
    send_hot = (sent_slots[:, :, None] == jnp.arange(node_count, dtype=jnp.int32)).astype(BF)
    outgoing = jnp.einsum(
        "khn,nd->khd", send_hot, node_latent, preferred_element_type=F32
    ).astype(BF)
    received = [
        lax.ppermute(outgoing[k], axis, pairs) for k, (axis, (pairs, _, _)) in enumerate(routes)
    ]
    node_table = jnp.concatenate([node_latent] + received, 0)
    block = (edge_sender - node_count) // halo_slots
    place = jnp.zeros_like(block)
    for k, (_, (_, _, taken)) in enumerate(routes):
        place = jnp.where(block == taken, k, place)
    sender = jnp.where(
        edge_sender < node_count, edge_sender, edge_sender + (place - block) * halo_slots
    )
    sender_hot = (sender[:, None] == jnp.arange(table_rows, dtype=jnp.int32)).astype(BF)
    receiver_hot = (edge_receiver[:, None] == jnp.arange(node_count, dtype=jnp.int32)).astype(BF)
    sender_rows = jnp.dot(sender_hot, node_table, preferred_element_type=F32).astype(BF)
    receiver_rows = jnp.dot(receiver_hot, node_latent, preferred_element_type=F32).astype(BF)
    inputs = jnp.concatenate([edge_latent, sender_rows, receiver_rows], 1)
    preact = jnp.dot(inputs, w_first, preferred_element_type=F32) + bias_first.astype(F32)
    activation = jax.nn.silu(preact).astype(BF)
    second_pre = jnp.dot(activation, w_second, preferred_element_type=F32) + bias_second.astype(F32)
    normalized, inv_std = norm_parts(second_pre)
    upstream = jnp.dot(receiver_hot, node_cotangent, preferred_element_type=F32)
    scaled = upstream * norm_gain.astype(F32)
    norm_back = (
        inv_std
        * (
            scaled
            - jnp.mean(scaled, -1, keepdims=True)
            - normalized * jnp.mean(scaled * normalized, -1, keepdims=True)
        )
    ).astype(BF)
    outer = (((0,), (0,)), ((), ()))
    second_grad = lax.dot_general(activation, norm_back, outer, preferred_element_type=F32)
    sigmoid_pre = jax.nn.sigmoid(preact)
    pre_back = (
        jnp.dot(norm_back, w_second.T, preferred_element_type=F32)
        * sigmoid_pre
        * (1.0 + preact * (1.0 - sigmoid_pre))
    ).astype(BF)
    first_grad = lax.dot_general(inputs, pre_back, outer, preferred_element_type=F32)
    input_back = jnp.dot(pre_back, w_first.T, preferred_element_type=F32)
    edge_grad = (upstream + input_back[:, :feature_width]).astype(BF)
    table_grad = contract(sender_hot, input_back[:, feature_width : 2 * feature_width])
    receiver_grad = contract(receiver_hot, input_back[:, 2 * feature_width :])
    halo_grad = table_grad[node_count:].reshape(blocks, halo_slots, feature_width).astype(BF)
    returned = jnp.stack(
        [
            lax.ppermute(halo_grad[k], axis, [(t, s) for s, t in pairs])
            for k, (axis, (pairs, _, _)) in enumerate(routes)
        ],
        0,
    )
    back = jnp.einsum("khn,khd->nd", send_hot, returned, preferred_element_type=F32)
    node_grad = (
        node_cotangent.astype(F32) + table_grad[:node_count] + receiver_grad + back
    ).astype(BF)
    first_weight_sq = jnp.sum(jnp.square(w_first.astype(F32)), 0)
    second_weight_sq = jnp.sum(jnp.square(w_second.astype(F32)), 0)
    first_share, second_share, first_grad_sq, second_grad_sq = reduce_weights(
        first_grad, second_grad
    )
    first_update = clip_share(first_share, first_grad_sq, first_weight_sq, w_first.shape[0])
    second_update = clip_share(second_share, second_grad_sq, second_weight_sq, w_second.shape[0])
    return (node_grad, edge_grad, first_update, second_update)


def solution(mesh):
    return jax.shard_map(
        per_device,
        mesh=mesh,
        in_specs=(
            P(("wide", "narrow"), None),
            P(("wide", "narrow"), None),
            P(("wide", "narrow"), None),
            P(),
            P(),
            P(),
            P(),
            P(),
            P(("wide", "narrow"), None, None),
            P(("wide", "narrow")),
            P(("wide", "narrow")),
        ),
        out_specs=(
            P(("wide", "narrow"), None),
            P(("wide", "narrow"), None),
            P("wide", None),
            P("wide", None),
        ),
        check_vma=False,
    )
```

```python
import functools
import math

import jax
import jax.numpy as jnp
from jax import lax
from jax.experimental import pallas as pl
from jax.experimental.pallas import tpu as pltpu
from jax.sharding import PartitionSpec as P

BF = jnp.bfloat16
F32 = jnp.float32


def halo_routes(axis, base, ring):
    count = lax.axis_size(axis)
    if count % 2:
        up = [(i, (i + 1) % count) for i in range(count) if ring or i + 1 < count]
        return [(up, base, base), ([(t, s) for s, t in up], base + 1, base + 1)]
    odd = lax.axis_index(axis) % 2
    near = [(i, i ^ 1) for i in range(count)]
    far = [(i, ((i + 1) ^ 1) - 1) for i in range(count)]
    far = [(s, t % count) for s, t in far if ring or 0 <= t < count]
    routes = [(near, base + odd, base + 1 - odd)]
    if far:
        routes.insert(0, (far, base + 1 - odd, base + odd))
    return routes


INNER = (((0,), (0,)), ((), ()))
OUTER = (((1,), (1,)), ((), ()))


def mm(left, right, dims=(((1,), (0,)), ((), ()))):
    return lax.dot_general(left, right, dims, preferred_element_type=F32)


def two_parts(values):
    high = values.astype(BF)
    return high, (values - high.astype(F32)).astype(BF)


def routes_of():
    routes = [("wide", r) for r in halo_routes("wide", 0, True)]
    return routes + [("narrow", r) for r in halo_routes("narrow", 2, False)]


def local_call(body, outs, args, gflops, far=0, scratch=()):
    vmem = pl.BlockSpec(memory_space=pltpu.VMEM)
    hbm = pl.BlockSpec(memory_space=pltpu.HBM)
    args = [
        pltpu.with_memory_space_constraint(value, pltpu.HBM) if i < far else value
        for i, value in enumerate(args)
    ]
    return pl.pallas_call(
        body,
        out_shape=outs,
        in_specs=[hbm] * far + [vmem] * (len(args) - far),
        out_specs=jax.tree.map(lambda _: vmem, outs),
        scratch_shapes=scratch,
        compiler_params=pltpu.CompilerParams(vmem_limit_bytes=VMEM_LIMIT),
        cost_estimate=pl.CostEstimate(
            flops=int(gflops * 1e9), bytes_accessed=1 << 20, transcendentals=0
        ),
    )(*args)


def fetch(sources, targets, sems):
    copies = [
        pltpu.make_async_copy(source, target, sems.at[i])
        for i, (source, target) in enumerate(zip(sources, targets))
    ]
    for copy in copies:
        copy.start()
    return copies


CHAINS = 2
VMEM_LIMIT = 24 * 1024 * 1024


def slot_hot(send_ref, block, node_count):
    slots = send_ref[0, pl.ds(block, 1), :]
    rows = lax.broadcasted_iota(jnp.int32, (node_count, slots.shape[1]), 0)
    return jnp.where(rows == slots, 1.0, 0.0).astype(BF)


def gather_body(send_hbm, node_hbm, send_ref, node_ref, *refs):
    *out_refs, sems = refs
    for copy in fetch((send_hbm, node_hbm), (send_ref, node_ref), sems):
        copy.wait()
    for (_, (_, sent, _)), out_ref in zip(routes_of(), out_refs):
        hot = slot_hot(send_ref, sent, node_ref.shape[0])
        out_ref[...] = mm(hot, node_ref[...], INNER).astype(BF)


def prepare_body(
    sender_hbm,
    receiver_hbm,
    cot_hbm,
    edge_hbm,
    w_first_hbm,
    w_second_hbm,
    node_ref,
    vectors_ref,
    start_ref,
    sender_hot_ref,
    receiver_hot_ref,
    edge_t_ref,
    up_ref,
    weight_sq_ref,
    cot_ref,
    w_first_ref,
    w_second_ref,
    sender_ref,
    receiver_ref,
    edge_ref,
    sems,
    *,
    slots,
):
    copies = fetch(
        (sender_hbm, receiver_hbm, cot_hbm, edge_hbm, w_first_hbm, w_second_hbm),
        (sender_ref, receiver_ref, cot_ref, edge_ref, w_first_ref, w_second_ref),
        sems,
    )
    nodes, width = node_ref.shape
    edges = edge_ref.shape[0]
    copies[0].wait()
    sender = sender_ref[...]
    row = sender
    for k, (_, (_, _, taken)) in enumerate(routes_of()):
        begin = nodes + taken * slots
        here = (sender >= begin) & (sender < begin + slots)
        row = jnp.where(here, sender - begin + (nodes + k * slots), row)
    table_rows = sender_hot_ref.shape[0]
    ids = lax.broadcasted_iota(jnp.int32, (table_rows, edges), 0)
    sender_hot_ref[...] = jnp.where(ids == row, 1.0, 0.0).astype(BF)
    copies[1].wait()
    ids = lax.broadcasted_iota(jnp.int32, (nodes, edges), 0)
    receiver_hot = jnp.where(ids == receiver_ref[...], 1.0, 0.0).astype(BF)
    receiver_hot_ref[...] = receiver_hot
    receiver_rows = mm(receiver_hot, node_ref[...], INNER).astype(BF)
    copies[2].wait()
    up_ref[...] = mm(receiver_hot, cot_ref[...], INNER).astype(BF)
    copies[3].wait()
    edge_t_ref[...] = edge_ref[...].T
    copies[4].wait()
    start_ref[...] = (
        mm(edge_ref[...], w_first_ref[:width])
        + mm(receiver_rows, w_first_ref[2 * width :])
        + vectors_ref[0:1]
    )
    first = w_first_ref[...].astype(F32)
    weight_sq_ref[0:1, :] = jnp.sum(first * first, 0, keepdims=True)
    copies[5].wait()
    second = w_second_ref[...].astype(F32)
    weight_sq_ref[1:2, :] = jnp.sum(second * second, 0, keepdims=True)


def middle_body(*refs, blocks, tile):
    (
        start_ref,
        sender_hot_ref,
        up_ref,
        node_ref,
        w_first_ref,
        w_second_ref,
        vectors_ref,
    ) = refs[:7]
    received = refs[7 : 7 + blocks]
    pre_back_ref, norm_back_ref, act_t_ref = refs[7 + blocks :]
    width = node_ref.shape[1]
    table = jnp.concatenate([node_ref[...]] + [r[...] for r in received], 0)
    bias, gain = vectors_ref[1:2], vectors_ref[2:3]
    for begin in range(0, start_ref.shape[0], tile):
        part = slice(begin, begin + tile)
        rows = mm(sender_hot_ref[:, part], table, INNER).astype(BF)
        preact = start_ref[part] + mm(rows, w_first_ref[width : 2 * width])
        sigma = 1.0 / (1.0 + jnp.exp(-preact))
        activation = (preact * sigma).astype(BF)
        act_t_ref[:, part] = activation.T
        second_pre = mm(activation, w_second_ref[...]) + bias
        centered = second_pre - jnp.mean(second_pre, -1, keepdims=True)
        variance = jnp.mean(centered * centered, -1, keepdims=True)
        inv_std = lax.rsqrt(variance + 1e-05)
        normalized = centered * inv_std
        scaled = up_ref[part].astype(F32) * gain
        norm_back = (
            inv_std
            * (
                scaled
                - jnp.mean(scaled, -1, keepdims=True)
                - normalized * jnp.mean(scaled * normalized, -1, keepdims=True)
            )
        ).astype(BF)
        norm_back_ref[part] = norm_back
        back = mm(norm_back, w_second_ref[...], OUTER)
        pre_back_ref[part] = (back * (sigma * (1.0 + preact * (1.0 - sigma)))).astype(BF)


def half_bit():
    narrow = lax.axis_size("narrow")
    return (lax.axis_index("narrow") // (narrow // 2)) % 2


def outer_body(*refs, blocks, own, chain):
    (edge_t_ref, act_t_ref, sender_hot_ref, receiver_hot_ref, pre_back_ref, norm_back_ref) = refs[:6]
    node_ref = refs[6]
    received = refs[7 : 7 + blocks]
    out_ref = refs[7 + blocks]
    span = out_ref.shape[2]
    half = half_bit() if own else 1 - half_bit()
    begin = pl.multiple_of(half * (CHAINS * span) + chain * span, span)
    columns = pl.ds(begin, span)
    pre_back = pre_back_ref[:, columns]
    node = node_ref[...]
    table = jnp.concatenate([node] + [r[...] for r in received], 0)
    by_sender = mm(sender_hot_ref[...], pre_back)
    by_receiver = mm(receiver_hot_ref[...], pre_back)
    high, low = two_parts(by_sender)
    high_r, low_r = two_parts(by_receiver)
    first = jnp.concatenate(
        [
            mm(edge_t_ref[...], pre_back),
            mm(table, high, INNER) + mm(table, low, INNER),
            mm(node, high_r, INNER) + mm(node, low_r, INNER),
        ],
        0,
    )
    second = mm(act_t_ref[...], norm_back_ref[:, columns])
    wide = out_ref.shape[0]
    first_rows = first.shape[0] // wide
    second_rows = second.shape[0] // wide
    for w in range(wide):
        out_ref[w, :first_rows] = first[w * first_rows : (w + 1) * first_rows].astype(out_ref.dtype)
        out_ref[w, first_rows:] = second[w * second_rows : (w + 1) * second_rows].astype(
            out_ref.dtype
        )


def back_body(*refs, blocks, slots):
    (pre_back_ref, w_first_ref, up_ref, cot_ref, sender_hot_ref, receiver_hot_ref) = refs[:6]
    edge_grad_ref, own_ref = refs[6:8]
    halo_refs = refs[8:]
    nodes, width = cot_ref.shape
    pre_back = pre_back_ref[...]
    high, low = two_parts(mm(sender_hot_ref[...], pre_back))
    weights = w_first_ref[width : 2 * width]
    table_grad = mm(high, weights, OUTER) + mm(low, weights, OUTER)
    for k, halo_ref in enumerate(halo_refs):
        begin = nodes + k * slots
        halo_ref[...] = table_grad[begin : begin + slots].astype(BF)
    high, low = two_parts(mm(receiver_hot_ref[...], pre_back))
    weights = w_first_ref[2 * width :]
    receiver_grad = mm(high, weights, OUTER) + mm(low, weights, OUTER)
    own_ref[...] = cot_ref[...].astype(F32) + table_grad[:nodes] + receiver_grad
    edge_grad_ref[...] = (
        up_ref[...].astype(F32) + mm(pre_back, w_first_ref[:width], OUTER)
    ).astype(BF)


def return_body(send_ref, own_ref, *refs):
    total = own_ref[...]
    for (_, (_, sent, _)), returned in zip(routes_of(), refs[:-1]):
        total += mm(slot_hot(send_ref, sent, total.shape[0]), returned[...])
    refs[-1][...] = total.astype(BF)


def combine_body(kept_ref, got_ref, next_ref, sent_ref, *, step):
    a = lax.axis_index("wide")
    odd = lax.axis_index("narrow") % 2
    low, high = a % 2, (a // 2) % 2
    for slot in range(next_ref.shape[0]):
        if step == 0:
            h, j = slot // 2, slot % 2
            kept = 4 * h + (1 - odd) * (2 * j + low) + odd * (2 * high + j)
            sent = 4 * h + (1 - odd) * (2 * j + 1 - low) + odd * (2 - 2 * high + j)
        elif step == 1:
            left = (1 - odd) * high + odd * low
            kept, sent = 2 * slot + left, 2 * slot + 1 - left
        else:
            bit = (a // (1 << step)) % 2
            kept, sent = 2 * slot + bit, 2 * slot + 1 - bit
        next_ref[slot] = kept_ref[kept] + got_ref[kept].astype(F32)
        sent_ref[slot] = (kept_ref[sent] + got_ref[sent].astype(F32)).astype(BF)


def whole_body(kept_ref, got_ref, next_ref, sent_ref):
    total = kept_ref[...] + got_ref[...].astype(F32)
    next_ref[...] = total
    sent_ref[...] = total.astype(BF)


def finish_body(kept_ref, got_ref, value_ref):
    value_ref[...] = kept_ref[...] + got_ref[...].astype(F32)


def sums_body(*refs, first_rows):
    value_ref, sums_ref = refs[2 * CHAINS :]
    for c in range(CHAINS):
        value = refs[c][...] + refs[CHAINS + c][...].astype(F32)
        columns = slice(c * value.shape[2], (c + 1) * value.shape[2])
        value_ref[:, :, columns] = value
        value = value * value
        sums_ref[0:1, columns] = jnp.sum(jnp.sum(value[:, :first_rows], 0), 0, keepdims=True)
        sums_ref[1:2, columns] = jnp.sum(jnp.sum(value[:, first_rows:], 0), 0, keepdims=True)


def clip_body(own_ref, other_ref, sums_ref, other_sums_ref, weight_sq_ref, first_ref, second_ref, *, top):
    half = half_bit()
    span = own_ref.shape[2]
    first_rows = first_ref.shape[0]
    share = lax.axis_index("wide") // top
    width = 2 * span
    wide = lax.axis_size("wide")
    columns = (
        pl.ds(pl.multiple_of(half * span, span), span),
        pl.ds(pl.multiple_of((1 - half) * span, span), span),
    )
    sums = (sums_ref[...] + 1e-06, other_sums_ref[...] + 1e-06)
    weight = [weight_sq_ref[:, c] + 1e-06 for c in columns]
    total = sum(jnp.sum(jnp.sqrt(s / w), 1, keepdims=True) for s, w in zip(sums, weight))
    mean_ratio = total / width
    fans = (first_ref.shape[0] * wide, second_ref.shape[0] * wide)
    for c, s, w, value_ref in zip(columns, sums, weight, (own_ref, other_ref)):
        factor = jnp.minimum(1.0 / (mean_ratio * jnp.sqrt(w)), 1.0 / jnp.sqrt(s))
        value = value_ref[share]
        first_ref[:, c] = value[:first_rows] * (factor[0:1] * math.sqrt(fans[0]))
        second_ref[:, c] = value[first_rows:] * (factor[1:2] * math.sqrt(fans[1]))


def swap_pairs(size, mask):
    return [(i, i ^ mask) for i in range(size)]


def crossed(value, even_mask, odd_mask):
    wide, narrow = lax.axis_size("wide"), lax.axis_size("narrow")
    pairs = []
    for i in range(wide):
        for j in range(narrow):
            pairs.append((i * narrow + j, (i ^ (odd_mask if j % 2 else even_mask)) * narrow + j))
    return lax.ppermute(value, ("wide", "narrow"), pairs)


def per_device(
    node_latent,
    edge_latent,
    node_cotangent,
    w_first,
    bias_first,
    w_second,
    bias_second,
    norm_gain,
    send_map,
    edge_sender,
    edge_receiver,
):
    nodes, width = node_latent.shape
    edges = edge_latent.shape[0]
    slots = send_map.shape[2]
    wide, narrow = lax.axis_size("wide"), lax.axis_size("narrow")
    if wide < 4 or wide & (wide - 1) or narrow < 2 or narrow & (narrow - 1):
        raise ValueError("axis sizes")
    routes = routes_of()
    blocks = len(routes)
    table_rows = nodes + blocks * slots

    def like(shape, kind):
        return jax.ShapeDtypeStruct(shape, kind)

    halo = [like((slots, width), BF)] * blocks
    send_slots, node, *outgoing = local_call(
        gather_body,
        [like(send_map.shape, jnp.int32), like((nodes, width), BF), *halo],
        (send_map, node_latent),
        0.1,
        far=2,
        scratch=[pltpu.SemaphoreType.DMA((2,))],
    )
    received = [
        lax.ppermute(block, axis, pairs) for block, (axis, (pairs, _, _)) in zip(outgoing, routes)
    ]
    vectors = jnp.stack([v.astype(F32) for v in (bias_first, bias_second, norm_gain)], 0)
    start, sender_hot, receiver_hot, edge_t, up, weight_sq, cot, weights, weights_2 = local_call(
        functools.partial(prepare_body, slots=slots),
        [
            like((edges, width), F32),
            like((table_rows, edges), BF),
            like((nodes, edges), BF),
            like((width, edges), BF),
            like((edges, width), BF),
            like((2, width), F32),
            like((nodes, width), BF),
            like(w_first.shape, BF),
            like(w_second.shape, BF),
        ],
        (
            edge_sender.reshape(1, edges),
            edge_receiver.reshape(1, edges),
            node_cotangent,
            edge_latent,
            w_first,
            w_second,
            node,
            vectors,
        ),
        1.0,
        far=6,
        scratch=[
            pltpu.VMEM((1, edges), jnp.int32),
            pltpu.VMEM((1, edges), jnp.int32),
            pltpu.VMEM((edges, width), BF),
            pltpu.SemaphoreType.DMA((6,)),
        ],
    )
    pre_back, norm_back, act_t = local_call(
        functools.partial(middle_body, blocks=blocks, tile=edges // 2),
        [like((edges, width), BF), like((edges, width), BF), like((width, edges), BF)],
        (start, sender_hot, up, node, weights, weights_2, vectors, *received),
        1.0,
    )
    first_rows, second_rows = w_first.shape[0] // wide, w_second.shape[0] // wide
    rows = first_rows + second_rows
    span = width // 2 // CHAINS
    operands = (edge_t, act_t, sender_hot, receiver_hot, pre_back, norm_back, node, *received)

    def outer(own, chain, kind):
        (grad,) = local_call(
            functools.partial(outer_body, blocks=blocks, own=own, chain=chain),
            [like((wide, rows, span), kind)],
            operands,
            0.6 / CHAINS,
        )
        return grad

    half_swap = swap_pairs(narrow, narrow // 2)
    gots = [lax.ppermute(outer(False, c, BF), "narrow", half_swap) for c in range(CHAINS)]
    kepts = [outer(True, c, F32) for c in range(CHAINS)]
    edge_grad, own_grad, *halo_grad = local_call(
        functools.partial(back_body, blocks=blocks, slots=slots),
        [like((edges, width), BF), like((nodes, width), F32), *halo],
        (pre_back, weights, up, cot, sender_hot, receiver_hot),
        1.0,
    )
    mask = narrow // 4
    while mask:
        span //= 2
        bit = (lax.axis_index("narrow") // mask) % 2
        for c in range(CHAINS):
            value = kepts[c] + gots[c].astype(F32)
            sent = lax.dynamic_slice_in_dim(value, (1 - bit) * span, span, 2).astype(BF)
            kepts[c] = lax.dynamic_slice_in_dim(value, bit * span, span, 2)
            gots[c] = lax.ppermute(sent, "narrow", swap_pairs(narrow, mask))
        mask //= 2
    bits = wide.bit_length() - 1
    for step in range(bits - 1):
        shape = (wide >> (step + 1), rows, span)
        masks = [(1, 2), (2, 1)][step] if step < 2 else (1 << step, 1 << step)
        for c in range(CHAINS):
            kepts[c], sent = local_call(
                functools.partial(combine_body, step=step),
                [like(shape, F32), like(shape, BF)],
                (kepts[c], gots[c]),
                0.01,
            )
            gots[c] = crossed(sent, *masks)
        if step == 0:
            gots[-1], halo_grad = lax.optimization_barrier((gots[-1], halo_grad))
            returned = [
                lax.ppermute(block, axis, [(t, s) for s, t in pairs])
                for block, (axis, (pairs, _, _)) in zip(halo_grad, routes)
            ]
        if step == bits - 2:
            gots[-1], returned = lax.optimization_barrier((gots[-1], returned))
    (node_grad,) = local_call(
        return_body, [like((nodes, width), BF)], (send_slots, own_grad, *returned), 0.1
    )
    top = wide // 2
    shape = (2, rows, span)
    for c in range(CHAINS):
        kepts[c], sent = local_call(
            whole_body, [like(shape, F32), like(shape, BF)], (kepts[c], gots[c]), 0.01
        )
        gots[c] = crossed(sent, top, top)
        if narrow > 2:
            (value,) = local_call(finish_body, [like(shape, F32)], (kepts[c], gots[c]), 0.01)
            mask = 1
            while mask < narrow // 2:
                other = lax.ppermute(value, "narrow", swap_pairs(narrow, mask))
                value = jnp.where(
                    (lax.axis_index("narrow") // mask) % 2 == 0,
                    jnp.concatenate([value, other], 2),
                    jnp.concatenate([other, value], 2),
                )
                mask *= 2
            kepts[c], gots[c] = value, jnp.zeros(value.shape, BF)
    value, sums = local_call(
        functools.partial(sums_body, first_rows=first_rows),
        [like((2, rows, width // 2), F32), like((2, width // 2), F32)],
        (*kepts, *gots),
        0.001,
    )
    other = lax.ppermute(value, "narrow", half_swap)
    for position in range(bits - 1):
        sums = sums + lax.ppermute(sums, "wide", swap_pairs(wide, 1 << position))
    other_sums = lax.ppermute(sums, "narrow", half_swap)
    first_update, second_update = local_call(
        functools.partial(clip_body, top=top),
        [like((first_rows, width), F32), like((second_rows, width), F32)],
        (value, other, sums, other_sums, weight_sq),
        0.001,
    )
    return (node_grad, edge_grad, first_update, second_update)


def solution(mesh):
    return jax.shard_map(
        per_device,
        mesh=mesh,
        in_specs=(
            P(("wide", "narrow"), None),
            P(("wide", "narrow"), None),
            P(("wide", "narrow"), None),
            P(),
            P(),
            P(),
            P(),
            P(),
            P(("wide", "narrow"), None, None),
            P(("wide", "narrow")),
            P(("wide", "narrow")),
        ),
        out_specs=(
            P(("wide", "narrow"), None),
            P(("wide", "narrow"), None),
            P("wide", None),
            P("wide", None),
        ),
        check_vma=False,
    )
```

```python
import functools
import math

import jax
import jax.numpy as jnp
from jax import lax
from jax.experimental import pallas as pl
from jax.experimental.pallas import tpu as pltpu
from jax.sharding import PartitionSpec as P


BF = jnp.bfloat16
F32 = jnp.float32


def halo_routes(axis, base, ring):
    count = lax.axis_size(axis)
    if count % 2:
        up = [(i, (i + 1) % count) for i in range(count) if ring or i + 1 < count]
        return [(up, base, base), ([(t, s) for s, t in up], base + 1, base + 1)]
    odd = lax.axis_index(axis) % 2
    near = [(i, i ^ 1) for i in range(count)]
    far = [(i, ((i + 1) ^ 1) - 1) for i in range(count)]
    far = [(s, t % count) for s, t in far if ring or 0 <= t < count]
    routes = [(near, base + odd, base + 1 - odd)]
    if far:
        routes.insert(0, (far, base + 1 - odd, base + odd))
    return routes


INNER = (((0,), (0,)), ((), ()))
OUTER = (((1,), (1,)), ((), ()))


def mm(left, right, dims=(((1,), (0,)), ((), ()))):
    return lax.dot_general(left, right, dims, preferred_element_type=F32)


def two_parts(values):
    high = values.astype(BF)
    return high, (values - high.astype(F32)).astype(BF)


def routes_of():
    routes = [("wide", r) for r in halo_routes("wide", 0, True)]
    return routes + [("narrow", r) for r in halo_routes("narrow", 2, False)]


def local_call(body, outs, args, gflops, far=0, scratch=()):
    vmem = pl.BlockSpec(memory_space=pltpu.VMEM)
    hbm = pl.BlockSpec(memory_space=pltpu.HBM)
    args = [
        pltpu.with_memory_space_constraint(value, pltpu.HBM) if i < far else value
        for i, value in enumerate(args)
    ]
    return pl.pallas_call(
        body,
        out_shape=outs,
        in_specs=[hbm] * far + [vmem] * (len(args) - far),
        out_specs=jax.tree.map(lambda _: vmem, outs),
        scratch_shapes=scratch,
        compiler_params=pltpu.CompilerParams(vmem_limit_bytes=VMEM_LIMIT),
        cost_estimate=pl.CostEstimate(
            flops=int(gflops * 1e9), bytes_accessed=1 << 20, transcendentals=0
        ),
    )(*args)


def fetch(sources, targets, sems):
    copies = [
        pltpu.make_async_copy(source, target, sems.at[i])
        for i, (source, target) in enumerate(zip(sources, targets))
    ]
    for copy in copies:
        copy.start()
    return copies


CHAINS = 2
TILES = 1
VMEM_LIMIT = 24 * 1024 * 1024


def slot_hot(send_ref, block, node_count):
    slots = send_ref[0, pl.ds(block, 1), :]
    rows = lax.broadcasted_iota(jnp.int32, (node_count, slots.shape[1]), 0)
    return jnp.where(rows == slots, 1.0, 0.0).astype(BF)


def gather_body(send_hbm, node_hbm, send_ref, node_ref, *refs):
    *out_refs, sems = refs
    for copy in fetch((send_hbm, node_hbm), (send_ref, node_ref), sems):
        copy.wait()
    for (_, (_, sent, _)), out_ref in zip(routes_of(), out_refs):
        hot = slot_hot(send_ref, sent, node_ref.shape[0])
        out_ref[...] = mm(hot, node_ref[...], INNER).astype(BF)


def prepare_body(
    sender_hbm,
    receiver_hbm,
    cot_hbm,
    edge_hbm,
    w_first_hbm,
    w_second_hbm,
    node_ref,
    vectors_ref,
    start_ref,
    sender_hot_ref,
    receiver_hot_ref,
    edge_t_ref,
    up_ref,
    weight_sq_ref,
    cot_ref,
    w_first_ref,
    w_second_ref,
    w_second_t_ref,
    sender_rows_ref,
    sender_ref,
    receiver_ref,
    edge_ref,
    sems,
    *,
    slots,
):
    copies = fetch(
        (sender_hbm, receiver_hbm, cot_hbm, edge_hbm, w_first_hbm, w_second_hbm),
        (sender_ref, receiver_ref, cot_ref, edge_ref, w_first_ref, w_second_ref),
        sems,
    )
    nodes, width = node_ref.shape
    edges = edge_ref.shape[0]
    copies[0].wait()
    sender = sender_ref[...]
    row = sender
    for k, (_, (_, _, taken)) in enumerate(routes_of()):
        begin = nodes + taken * slots
        here = (sender >= begin) & (sender < begin + slots)
        row = jnp.where(here, sender - begin + (nodes + k * slots), row)
    table_rows = sender_hot_ref.shape[0]
    ids = lax.broadcasted_iota(jnp.int32, (table_rows, edges), 0)
    sender_hot = jnp.where(ids == row, 1.0, 0.0).astype(BF)
    sender_hot_ref[...] = sender_hot
    sender_rows_ref[...] = sender_hot.T
    copies[1].wait()
    ids = lax.broadcasted_iota(jnp.int32, (nodes, edges), 0)
    receiver_hot = jnp.where(ids == receiver_ref[...], 1.0, 0.0).astype(BF)
    receiver_hot_ref[...] = receiver_hot
    receiver_rows = mm(receiver_hot, node_ref[...], INNER).astype(BF)
    copies[2].wait()
    up_ref[...] = mm(receiver_hot, cot_ref[...], INNER).astype(BF)
    copies[3].wait()
    edge_t_ref[...] = edge_ref[...].T
    copies[4].wait()
    start_ref[...] = (
        mm(edge_ref[...], w_first_ref[:width])
        + mm(receiver_rows, w_first_ref[2 * width :])
        + vectors_ref[0:1]
    )
    first = w_first_ref[...].astype(F32)
    weight_sq_ref[0:1, :] = jnp.sum(first * first, 0, keepdims=True)
    copies[5].wait()
    w_second_t_ref[...] = w_second_ref[...].T
    second = w_second_ref[...].astype(F32)
    weight_sq_ref[1:2, :] = jnp.sum(second * second, 0, keepdims=True)


def middle_body(*refs, blocks, tile):
    (
        start_ref,
        sender_rows_ref,
        up_ref,
        node_ref,
        w_first_ref,
        w_second_ref,
        w_second_t_ref,
        vectors_ref,
    ) = refs[:8]
    received = refs[8 : 8 + blocks]
    pre_back_ref, norm_back_ref, act_t_ref = refs[8 + blocks :]
    width = node_ref.shape[1]
    table = jnp.concatenate([node_ref[...]] + [r[...] for r in received], 0)
    bias, gain = vectors_ref[1:2], vectors_ref[2:3]
    for begin in range(0, start_ref.shape[0], tile):
        part = slice(begin, begin + tile)
        rows = mm(sender_rows_ref[part], table).astype(BF)
        preact = start_ref[part] + mm(rows, w_first_ref[width : 2 * width])
        sigma = 1.0 / (1.0 + jnp.exp(-preact))
        activation = (preact * sigma).astype(BF)
        act_t_ref[:, part] = activation.T
        second_pre = mm(activation, w_second_ref[...]) + bias
        centered = second_pre - jnp.mean(second_pre, -1, keepdims=True)
        variance = jnp.mean(centered * centered, -1, keepdims=True)
        inv_std = lax.rsqrt(variance + 1e-05)
        normalized = centered * inv_std
        scaled = up_ref[part].astype(F32) * gain
        norm_back = (
            inv_std
            * (
                scaled
                - jnp.mean(scaled, -1, keepdims=True)
                - normalized * jnp.mean(scaled * normalized, -1, keepdims=True)
            )
        ).astype(BF)
        norm_back_ref[part] = norm_back
        back = mm(norm_back, w_second_t_ref[...])
        pre_back_ref[part] = (back * (sigma * (1.0 + preact * (1.0 - sigma)))).astype(BF)


def half_bit():
    narrow = lax.axis_size("narrow")
    return (lax.axis_index("narrow") // (narrow // 2)) % 2


def outer_body(*refs, blocks, own):
    (edge_t_ref, act_t_ref, sender_hot_ref, receiver_hot_ref, pre_back_ref, norm_back_ref) = refs[:6]
    node_ref = refs[6]
    received = refs[7 : 7 + blocks]
    out_refs = refs[7 + blocks :]
    wide, _, span = out_refs[0].shape
    width = CHAINS * span
    half = half_bit() if own else 1 - half_bit()
    columns = pl.ds(pl.multiple_of(half * width, width), width)
    pre_back = pre_back_ref[:, columns]
    node = node_ref[...]
    table = jnp.concatenate([node] + [r[...] for r in received], 0)
    by_sender = mm(sender_hot_ref[...], pre_back)
    by_receiver = mm(receiver_hot_ref[...], pre_back)
    high, low = two_parts(by_sender)
    high_r, low_r = two_parts(by_receiver)
    first = jnp.concatenate(
        [
            mm(edge_t_ref[...], pre_back),
            mm(table, high, INNER) + mm(table, low, INNER),
            mm(node, high_r, INNER) + mm(node, low_r, INNER),
        ],
        0,
    )
    second = mm(act_t_ref[...], norm_back_ref[:, columns])
    first_rows = first.shape[0] // wide
    second_rows = second.shape[0] // wide
    for c, out_ref in enumerate(out_refs):
        part = slice(c * span, (c + 1) * span)
        for w in range(wide):
            block = first[w * first_rows : (w + 1) * first_rows, part]
            out_ref[w, :first_rows] = block.astype(out_ref.dtype)
            block = second[w * second_rows : (w + 1) * second_rows, part]
            out_ref[w, first_rows:] = block.astype(out_ref.dtype)


def back_body(*refs, blocks, slots):
    (pre_back_ref, w_first_ref, up_ref, cot_ref, sender_hot_ref, receiver_hot_ref) = refs[:6]
    edge_grad_ref, own_ref = refs[6:8]
    halo_refs = refs[8:]
    nodes, width = cot_ref.shape
    pre_back = pre_back_ref[...]
    high, low = two_parts(mm(sender_hot_ref[...], pre_back))
    weights = w_first_ref[width : 2 * width]
    table_grad = mm(high, weights, OUTER) + mm(low, weights, OUTER)
    for k, halo_ref in enumerate(halo_refs):
        begin = nodes + k * slots
        halo_ref[...] = table_grad[begin : begin + slots].astype(BF)
    high, low = two_parts(mm(receiver_hot_ref[...], pre_back))
    weights = w_first_ref[2 * width :]
    receiver_grad = mm(high, weights, OUTER) + mm(low, weights, OUTER)
    own_ref[...] = cot_ref[...].astype(F32) + table_grad[:nodes] + receiver_grad
    edge_grad_ref[...] = (
        up_ref[...].astype(F32) + mm(pre_back, w_first_ref[:width], OUTER)
    ).astype(BF)


def return_body(send_ref, own_ref, *refs):
    total = own_ref[...]
    for (_, (_, sent, _)), returned in zip(routes_of(), refs[:-1]):
        total += mm(slot_hot(send_ref, sent, total.shape[0]), returned[...])
    refs[-1][...] = total.astype(BF)


def combine_body(kept_ref, got_ref, next_ref, sent_ref, *, step):
    a = lax.axis_index("wide")
    odd = lax.axis_index("narrow") % 2
    low, high = a % 2, (a // 2) % 2
    for slot in range(next_ref.shape[0]):
        if step == 0:
            h, j = slot // 2, slot % 2
            kept = 4 * h + (1 - odd) * (2 * j + low) + odd * (2 * high + j)
            sent = 4 * h + (1 - odd) * (2 * j + 1 - low) + odd * (2 - 2 * high + j)
        elif step == 1:
            left = (1 - odd) * high + odd * low
            kept, sent = 2 * slot + left, 2 * slot + 1 - left
        else:
            bit = (a // (1 << step)) % 2
            kept, sent = 2 * slot + bit, 2 * slot + 1 - bit
        next_ref[slot] = kept_ref[kept] + got_ref[kept].astype(F32)
        sent_ref[slot] = (kept_ref[sent] + got_ref[sent].astype(F32)).astype(BF)


def whole_body(kept_ref, got_ref, next_ref, sent_ref):
    total = kept_ref[...] + got_ref[...].astype(F32)
    next_ref[...] = total
    sent_ref[...] = total.astype(BF)


def finish_body(kept_ref, got_ref, value_ref):
    value_ref[...] = kept_ref[...] + got_ref[...].astype(F32)


def sums_body(*refs, first_rows):
    value_ref, sums_ref = refs[2 * CHAINS :]
    for c in range(CHAINS):
        value = refs[c][...] + refs[CHAINS + c][...].astype(F32)
        columns = slice(c * value.shape[2], (c + 1) * value.shape[2])
        value_ref[:, :, columns] = value
        value = value * value
        sums_ref[0:1, columns] = jnp.sum(jnp.sum(value[:, :first_rows], 0), 0, keepdims=True)
        sums_ref[1:2, columns] = jnp.sum(jnp.sum(value[:, first_rows:], 0), 0, keepdims=True)


def clip_body(own_ref, other_ref, sums_ref, other_sums_ref, weight_sq_ref, first_ref, second_ref, *, top):
    half = half_bit()
    span = own_ref.shape[2]
    first_rows = first_ref.shape[0]
    share = lax.axis_index("wide") // top
    width = 2 * span
    wide = lax.axis_size("wide")
    columns = (
        pl.ds(pl.multiple_of(half * span, span), span),
        pl.ds(pl.multiple_of((1 - half) * span, span), span),
    )
    sums = (sums_ref[...] + 1e-06, other_sums_ref[...] + 1e-06)
    weight = [weight_sq_ref[:, c] + 1e-06 for c in columns]
    total = sum(jnp.sum(jnp.sqrt(s / w), 1, keepdims=True) for s, w in zip(sums, weight))
    mean_ratio = total / width
    fans = (first_ref.shape[0] * wide, second_ref.shape[0] * wide)
    for c, s, w, value_ref in zip(columns, sums, weight, (own_ref, other_ref)):
        factor = jnp.minimum(1.0 / (mean_ratio * jnp.sqrt(w)), 1.0 / jnp.sqrt(s))
        value = value_ref[share]
        first_ref[:, c] = value[:first_rows] * (factor[0:1] * math.sqrt(fans[0]))
        second_ref[:, c] = value[first_rows:] * (factor[1:2] * math.sqrt(fans[1]))


def swap_pairs(size, mask):
    return [(i, i ^ mask) for i in range(size)]


def crossed(value, even_mask, odd_mask):
    wide, narrow = lax.axis_size("wide"), lax.axis_size("narrow")
    pairs = []
    for i in range(wide):
        for j in range(narrow):
            pairs.append((i * narrow + j, (i ^ (odd_mask if j % 2 else even_mask)) * narrow + j))
    return lax.ppermute(value, ("wide", "narrow"), pairs)


def device_step(
    node_latent,
    edge_latent,
    node_cotangent,
    w_first,
    bias_first,
    w_second,
    bias_second,
    norm_gain,
    send_map,
    edge_sender,
    edge_receiver,
):
    nodes, width = node_latent.shape
    edges = edge_latent.shape[0]
    slots = send_map.shape[2]
    wide, narrow = lax.axis_size("wide"), lax.axis_size("narrow")
    if wide < 4 or wide & (wide - 1) or narrow < 2 or narrow & (narrow - 1):
        raise ValueError("axis sizes")
    routes = routes_of()
    blocks = len(routes)
    table_rows = nodes + blocks * slots

    def like(shape, kind):
        return jax.ShapeDtypeStruct(shape, kind)

    halo = [like((slots, width), BF)] * blocks
    send_slots, node, *outgoing = local_call(
        gather_body,
        [like(send_map.shape, jnp.int32), like((nodes, width), BF), *halo],
        (send_map, node_latent),
        0.1,
        far=2,
        scratch=[pltpu.SemaphoreType.DMA((2,))],
    )
    received = [
        lax.ppermute(block, axis, pairs) for block, (axis, (pairs, _, _)) in zip(outgoing, routes)
    ]
    vectors = jnp.stack([v.astype(F32) for v in (bias_first, bias_second, norm_gain)], 0)
    start, sender_hot, receiver_hot, edge_t, up, weight_sq, cot, weights, weights_2, weights_2t, sender_rows = local_call(
        functools.partial(prepare_body, slots=slots),
        [
            like((edges, width), F32),
            like((table_rows, edges), BF),
            like((nodes, edges), BF),
            like((width, edges), BF),
            like((edges, width), BF),
            like((2, width), F32),
            like((nodes, width), BF),
            like(w_first.shape, BF),
            like(w_second.shape, BF),
            like(w_second.shape[::-1], BF),
            like((edges, table_rows), BF),
        ],
        (
            edge_sender.reshape(1, edges),
            edge_receiver.reshape(1, edges),
            node_cotangent,
            edge_latent,
            w_first,
            w_second,
            node,
            vectors,
        ),
        1.0,
        far=6,
        scratch=[
            pltpu.VMEM((1, edges), jnp.int32),
            pltpu.VMEM((1, edges), jnp.int32),
            pltpu.VMEM((edges, width), BF),
            pltpu.SemaphoreType.DMA((6,)),
        ],
    )
    pre_back, norm_back, act_t = local_call(
        functools.partial(middle_body, blocks=blocks, tile=edges // TILES),
        [like((edges, width), BF), like((edges, width), BF), like((width, edges), BF)],
        (start, sender_rows, up, node, weights, weights_2, weights_2t, vectors, *received),
        1.0,
    )
    first_rows, second_rows = w_first.shape[0] // wide, w_second.shape[0] // wide
    rows = first_rows + second_rows
    span = width // 2 // CHAINS
    operands = (edge_t, act_t, sender_hot, receiver_hot, pre_back, norm_back, node, *received)

    def outer(own, kind):
        return local_call(
            functools.partial(outer_body, blocks=blocks, own=own),
            [like((wide, rows, span), kind)] * CHAINS,
            operands,
            0.6,
        )

    half_swap = swap_pairs(narrow, narrow // 2)
    gots = [lax.ppermute(sent, "narrow", half_swap) for sent in outer(False, BF)]
    kepts = list(outer(True, F32))
    edge_grad, own_grad, *halo_grad = local_call(
        functools.partial(back_body, blocks=blocks, slots=slots),
        [like((edges, width), BF), like((nodes, width), F32), *halo],
        (pre_back, weights, up, cot, sender_hot, receiver_hot),
        1.0,
    )
    mask = narrow // 4
    while mask:
        span //= 2
        bit = (lax.axis_index("narrow") // mask) % 2
        for c in range(CHAINS):
            value = kepts[c] + gots[c].astype(F32)
            sent = lax.dynamic_slice_in_dim(value, (1 - bit) * span, span, 2).astype(BF)
            kepts[c] = lax.dynamic_slice_in_dim(value, bit * span, span, 2)
            gots[c] = lax.ppermute(sent, "narrow", swap_pairs(narrow, mask))
        mask //= 2
    bits = wide.bit_length() - 1
    for step in range(bits - 1):
        shape = (wide >> (step + 1), rows, span)
        masks = [(1, 2), (2, 1)][step] if step < 2 else (1 << step, 1 << step)
        for c in range(CHAINS):
            kepts[c], sent = local_call(
                functools.partial(combine_body, step=step),
                [like(shape, F32), like(shape, BF)],
                (kepts[c], gots[c]),
                0.01,
            )
            gots[c] = crossed(sent, *masks)
    top = wide // 2
    shape = (2, rows, span)
    for c in range(CHAINS):
        kepts[c], sent = local_call(
            whole_body, [like(shape, F32), like(shape, BF)], (kepts[c], gots[c]), 0.01
        )
        gots[c] = crossed(sent, top, top)
        if narrow > 2:
            (value,) = local_call(finish_body, [like(shape, F32)], (kepts[c], gots[c]), 0.01)
            mask = 1
            while mask < narrow // 2:
                other = lax.ppermute(value, "narrow", swap_pairs(narrow, mask))
                value = jnp.where(
                    (lax.axis_index("narrow") // mask) % 2 == 0,
                    jnp.concatenate([value, other], 2),
                    jnp.concatenate([other, value], 2),
                )
                mask *= 2
            kepts[c], gots[c] = value, jnp.zeros(value.shape, BF)
    returned = []
    for block, (axis, (pairs, _, _)) in zip(halo_grad, routes):
        returned.append(lax.ppermute(block, axis, [(t, s) for s, t in pairs]))
    (node_grad,) = local_call(
        return_body, [like((nodes, width), BF)], (send_slots, own_grad, *returned), 0.1
    )
    value, sums = local_call(
        functools.partial(sums_body, first_rows=first_rows),
        [like((2, rows, width // 2), F32), like((2, width // 2), F32)],
        (*kepts, *gots),
        0.001,
    )
    other = lax.ppermute(value, "narrow", half_swap)
    for position in range(bits - 1):
        arrived = lax.ppermute(sums, "wide", swap_pairs(wide, 1 << position))
        sums = sums + arrived
    other_sums = lax.ppermute(sums, "narrow", half_swap)
    first_update, second_update = local_call(
        functools.partial(clip_body, top=top),
        [like((first_rows, width), F32), like((second_rows, width), F32)],
        (value, other, sums, other_sums, weight_sq),
        0.001,
    )
    return (node_grad, edge_grad, first_update, second_update)


def solution(mesh):
    return jax.shard_map(
        device_step,
        mesh=mesh,
        in_specs=(
            P(("wide", "narrow"), None),
            P(("wide", "narrow"), None),
            P(("wide", "narrow"), None),
            P(),
            P(),
            P(),
            P(),
            P(),
            P(("wide", "narrow"), None, None),
            P(("wide", "narrow")),
            P(("wide", "narrow")),
        ),
        out_specs=(
            P(("wide", "narrow"), None),
            P(("wide", "narrow"), None),
            P("wide", None),
            P("wide", None),
        ),
        check_vma=False,
    )
```

```python
import functools
import math

import jax
import jax.numpy as jnp
from jax import lax
from jax.experimental import pallas as pl
from jax.experimental.pallas import tpu as pltpu
from jax.sharding import PartitionSpec as P


BF = jnp.bfloat16
F32 = jnp.float32


def halo_routes(axis, base, ring):
    count = lax.axis_size(axis)
    if count % 2:
        up = [(i, (i + 1) % count) for i in range(count) if ring or i + 1 < count]
        return [(up, base, base), ([(t, s) for s, t in up], base + 1, base + 1)]
    odd = lax.axis_index(axis) % 2
    near = [(i, i ^ 1) for i in range(count)]
    far = [(i, ((i + 1) ^ 1) - 1) for i in range(count)]
    far = [(s, t % count) for s, t in far if ring or 0 <= t < count]
    routes = [(near, base + odd, base + 1 - odd)]
    if far:
        routes.insert(0, (far, base + 1 - odd, base + odd))
    return routes


INNER = (((0,), (0,)), ((), ()))
OUTER = (((1,), (1,)), ((), ()))


def mm(left, right, dims=(((1,), (0,)), ((), ()))):
    return lax.dot_general(left, right, dims, preferred_element_type=F32)


def two_parts(values):
    high = values.astype(BF)
    return high, (values - high.astype(F32)).astype(BF)


def routes_of():
    routes = [("wide", r) for r in halo_routes("wide", 0, True)]
    return routes + [("narrow", r) for r in halo_routes("narrow", 2, False)]


def local_call(body, outs, args, gflops, far=0, scratch=()):
    vmem = pl.BlockSpec(memory_space=pltpu.VMEM)
    hbm = pl.BlockSpec(memory_space=pltpu.HBM)
    args = [
        pltpu.with_memory_space_constraint(value, pltpu.HBM) if i < far else value
        for i, value in enumerate(args)
    ]
    return pl.pallas_call(
        body,
        out_shape=outs,
        in_specs=[hbm] * far + [vmem] * (len(args) - far),
        out_specs=jax.tree.map(lambda _: vmem, outs),
        scratch_shapes=scratch,
        compiler_params=pltpu.CompilerParams(vmem_limit_bytes=VMEM_LIMIT),
        cost_estimate=pl.CostEstimate(
            flops=int(gflops * 1e9), bytes_accessed=1 << 20, transcendentals=0
        ),
    )(*args)


def fetch(sources, targets, sems):
    copies = [
        pltpu.make_async_copy(source, target, sems.at[i])
        for i, (source, target) in enumerate(zip(sources, targets))
    ]
    for copy in copies:
        copy.start()
    return copies


CHAINS = 2
VMEM_LIMIT = 24 * 1024 * 1024


def slot_hot(send_ref, block, node_count):
    slots = send_ref[0, pl.ds(block, 1), :]
    rows = lax.broadcasted_iota(jnp.int32, (node_count, slots.shape[1]), 0)
    return jnp.where(rows == slots, 1.0, 0.0).astype(BF)


def gather_body(send_hbm, node_hbm, send_ref, node_ref, *refs):
    *out_refs, sems = refs
    for copy in fetch((send_hbm, node_hbm), (send_ref, node_ref), sems):
        copy.wait()
    for (_, (_, sent, _)), out_ref in zip(routes_of(), out_refs):
        hot = slot_hot(send_ref, sent, node_ref.shape[0])
        out_ref[...] = mm(hot, node_ref[...], INNER).astype(BF)


def prepare_body(
    sender_hbm,
    receiver_hbm,
    cot_hbm,
    edge_hbm,
    w_first_hbm,
    w_second_hbm,
    bias_hbm,
    bias_2_hbm,
    gain_hbm,
    node_ref,
    start_ref,
    sender_hot_ref,
    receiver_hot_ref,
    edge_t_ref,
    up_ref,
    weight_sq_ref,
    cot_ref,
    w_first_ref,
    w_second_ref,
    w_second_t_ref,
    near_rows_ref,
    far_rows_ref,
    vectors_ref,
    sender_ref,
    receiver_ref,
    edge_ref,
    bias_ref,
    bias_2_ref,
    gain_ref,
    sems,
    *,
    slots,
):
    copies = fetch(
        (sender_hbm, receiver_hbm, cot_hbm, edge_hbm, w_first_hbm, w_second_hbm, bias_hbm, bias_2_hbm, gain_hbm),
        (sender_ref, receiver_ref, cot_ref, edge_ref, w_first_ref, w_second_ref, bias_ref, bias_2_ref, gain_ref),
        sems,
    )
    nodes, width = node_ref.shape
    edges = edge_ref.shape[0]
    copies[0].wait()
    sender = sender_ref[...]
    row = sender
    for k, (_, (_, _, taken)) in enumerate(routes_of()):
        begin = nodes + taken * slots
        here = (sender >= begin) & (sender < begin + slots)
        row = jnp.where(here, sender - begin + (nodes + k * slots), row)
    table_rows = sender_hot_ref.shape[0]
    ids = lax.broadcasted_iota(jnp.int32, (table_rows, edges), 0)
    sender_hot = jnp.where(ids == row, 1.0, 0.0).astype(BF)
    sender_hot_ref[...] = sender_hot
    late = nodes + 2 * slots
    far_hot = sender_hot[nodes:late]
    near_rows_ref[...] = jnp.concatenate([sender_hot[:nodes], sender_hot[late:]], 0).T
    far_rows_ref[...] = jnp.concatenate([far_hot, far_hot], 0).T
    copies[1].wait()
    ids = lax.broadcasted_iota(jnp.int32, (nodes, edges), 0)
    receiver_hot = jnp.where(ids == receiver_ref[...], 1.0, 0.0).astype(BF)
    receiver_hot_ref[...] = receiver_hot
    receiver_rows = mm(receiver_hot, node_ref[...], INNER).astype(BF)
    copies[2].wait()
    up_ref[...] = mm(receiver_hot, cot_ref[...], INNER).astype(BF)
    copies[3].wait()
    edge_t_ref[...] = edge_ref[...].T
    copies[4].wait()
    for copy in copies[6:]:
        copy.wait()
    vectors_ref[0:1] = bias_2_ref[...].astype(F32).reshape(1, width)
    vectors_ref[1:2] = gain_ref[...].astype(F32).reshape(1, width)
    start_ref[...] = (
        mm(edge_ref[...], w_first_ref[:width])
        + mm(receiver_rows, w_first_ref[2 * width :])
        + bias_ref[...].astype(F32).reshape(1, width)
    )
    first = w_first_ref[...].astype(F32)
    weight_sq_ref[0:1, :] = jnp.sum(first * first, 0, keepdims=True)
    copies[5].wait()
    w_second_t_ref[...] = w_second_ref[...].T
    second = w_second_ref[...].astype(F32)
    weight_sq_ref[1:2, :] = jnp.sum(second * second, 0, keepdims=True)


def near_body(start_ref, near_rows_ref, up_ref, node_ref, w_first_ref, vectors_ref, *refs):
    *received, next_ref, scaled_ref = refs
    width = node_ref.shape[1]
    table = jnp.concatenate([node_ref[...]] + [r[...] for r in received], 0)
    rows = mm(near_rows_ref[...], table).astype(BF)
    next_ref[...] = start_ref[...] + mm(rows, w_first_ref[width : 2 * width])
    scaled = up_ref[...].astype(F32) * vectors_ref[1:2]
    scaled_ref[...] = scaled - jnp.mean(scaled, -1, keepdims=True)


def middle_body(
    start_ref,
    far_rows_ref,
    scaled_ref,
    far_ref,
    far_2_ref,
    w_first_ref,
    w_second_ref,
    w_second_t_ref,
    vectors_ref,
    pre_back_ref,
    norm_back_ref,
    act_t_ref,
):
    width = far_ref.shape[1]
    far = jnp.concatenate([far_ref[...], far_2_ref[...]], 0)
    far = jnp.concatenate(two_parts(mm(far, w_first_ref[width : 2 * width])), 0)
    preact = start_ref[...] + mm(far_rows_ref[...], far)
    sigma = 0.5 + 0.5 * jnp.tanh(0.5 * preact)
    activation = (preact * sigma).astype(BF)
    act_t_ref[...] = activation.T
    second_pre = mm(activation, w_second_ref[...]) + vectors_ref[0:1]
    centered = second_pre - jnp.mean(second_pre, -1, keepdims=True)
    variance = jnp.mean(centered * centered, -1, keepdims=True)
    inv_std = lax.rsqrt(variance + 1e-05)
    normalized = centered * inv_std
    scaled = scaled_ref[...]
    norm_back = (
        inv_std * (scaled - normalized * jnp.mean(scaled * normalized, -1, keepdims=True))
    ).astype(BF)
    norm_back_ref[...] = norm_back
    back = mm(norm_back, w_second_t_ref[...])
    pre_back_ref[...] = (back * (sigma * (1.0 + preact * (1.0 - sigma)))).astype(BF)


def chain_cuts(rows):
    cuts = [round(rows * c / CHAINS / 16) * 16 for c in range(CHAINS)] + [rows]
    return list(zip(cuts[:-1], cuts[1:]))


def half_bit():
    narrow = lax.axis_size("narrow")
    return (lax.axis_index("narrow") // (narrow // 2)) % 2


def outer_body(*refs, blocks, own):
    (edge_t_ref, act_t_ref, sender_hot_ref, receiver_hot_ref, pre_back_ref, norm_back_ref) = refs[:6]
    node_ref = refs[6]
    received = refs[7 : 7 + blocks]
    out_refs = refs[7 + blocks :]
    wide, _, width = out_refs[0].shape
    half = half_bit() if own else 1 - half_bit()
    columns = pl.ds(pl.multiple_of(half * width, width), width)
    pre_back = pre_back_ref[:, columns]
    node = node_ref[...]
    table = jnp.concatenate([node] + [r[...] for r in received], 0)
    by_sender = mm(sender_hot_ref[...], pre_back)
    by_receiver = mm(receiver_hot_ref[...], pre_back)
    high, low = two_parts(by_sender)
    high_r, low_r = two_parts(by_receiver)
    first = jnp.concatenate(
        [
            mm(edge_t_ref[...], pre_back),
            mm(table, high, INNER) + mm(table, low, INNER),
            mm(node, high_r, INNER) + mm(node, low_r, INNER),
        ],
        0,
    )
    second = mm(act_t_ref[...], norm_back_ref[:, columns])
    first_rows = first.shape[0] // wide
    second_rows = second.shape[0] // wide
    for (begin, end), out_ref in zip(chain_cuts(first_rows + second_rows), out_refs):
        inner = min(max(first_rows, begin), end)
        for w in range(wide):
            if begin < inner:
                block = first[w * first_rows + begin : w * first_rows + inner]
                out_ref[w, : inner - begin] = block.astype(out_ref.dtype)
            if inner < end:
                offset = w * second_rows - first_rows
                block = second[offset + inner : offset + end]
                out_ref[w, inner - begin :] = block.astype(out_ref.dtype)


def back_body(*refs, blocks, slots):
    (pre_back_ref, w_first_ref, up_ref, cot_ref, sender_hot_ref, receiver_hot_ref) = refs[:6]
    edge_grad_ref, own_ref = refs[6:8]
    halo_refs = refs[8:]
    nodes, width = cot_ref.shape
    pre_back = pre_back_ref[...]
    high, low = two_parts(mm(sender_hot_ref[...], pre_back))
    weights = w_first_ref[width : 2 * width]
    table_grad = mm(high, weights, OUTER) + mm(low, weights, OUTER)
    for k, halo_ref in enumerate(halo_refs):
        begin = nodes + k * slots
        halo_ref[...] = table_grad[begin : begin + slots].astype(BF)
    high, low = two_parts(mm(receiver_hot_ref[...], pre_back))
    weights = w_first_ref[2 * width :]
    receiver_grad = mm(high, weights, OUTER) + mm(low, weights, OUTER)
    own_ref[...] = cot_ref[...].astype(F32) + table_grad[:nodes] + receiver_grad
    edge_grad_ref[...] = (
        up_ref[...].astype(F32) + mm(pre_back, w_first_ref[:width], OUTER)
    ).astype(BF)


def return_body(send_ref, own_ref, *refs):
    total = own_ref[...]
    for (_, (_, sent, _)), returned in zip(routes_of(), refs[:-1]):
        total += mm(slot_hot(send_ref, sent, total.shape[0]), returned[...])
    refs[-1][...] = total.astype(BF)


def combine_body(kept_ref, got_ref, next_ref, sent_ref, *, step):
    a = lax.axis_index("wide")
    odd = lax.axis_index("narrow") % 2
    low, high = a % 2, (a // 2) % 2
    for slot in range(next_ref.shape[0]):
        if step == 0:
            h, j = slot // 2, slot % 2
            kept = 4 * h + (1 - odd) * (2 * j + low) + odd * (2 * high + j)
            sent = 4 * h + (1 - odd) * (2 * j + 1 - low) + odd * (2 - 2 * high + j)
        elif step == 1:
            left = (1 - odd) * high + odd * low
            kept, sent = 2 * slot + left, 2 * slot + 1 - left
        else:
            bit = (a // (1 << step)) % 2
            kept, sent = 2 * slot + bit, 2 * slot + 1 - bit
        next_ref[slot] = kept_ref[kept] + got_ref[kept].astype(F32)
        sent_ref[slot] = (kept_ref[sent] + got_ref[sent].astype(F32)).astype(BF)


def whole_body(kept_ref, got_ref, next_ref, sent_ref):
    total = kept_ref[...] + got_ref[...].astype(F32)
    next_ref[...] = total
    sent_ref[...] = total.astype(BF)


def finish_body(kept_ref, got_ref, value_ref):
    value_ref[...] = kept_ref[...] + got_ref[...].astype(F32)


def sums_body(*refs, first_rows):
    value_ref, sums_ref = refs[2 * CHAINS :]
    for c, (begin, end) in enumerate(chain_cuts(value_ref.shape[1])):
        value_ref[:, begin:end] = refs[c][...] + refs[CHAINS + c][...].astype(F32)
    value = value_ref[...]
    value = value * value
    sums_ref[0:1, :] = jnp.sum(jnp.sum(value[:, :first_rows], 0), 0, keepdims=True)
    sums_ref[1:2, :] = jnp.sum(jnp.sum(value[:, first_rows:], 0), 0, keepdims=True)


def clip_body(own_ref, other_ref, sums_ref, other_sums_ref, weight_sq_ref, first_ref, second_ref, *, top):
    half = half_bit()
    span = own_ref.shape[2]
    first_rows = first_ref.shape[0]
    share = lax.axis_index("wide") // top
    width = 2 * span
    wide = lax.axis_size("wide")
    columns = (
        pl.ds(pl.multiple_of(half * span, span), span),
        pl.ds(pl.multiple_of((1 - half) * span, span), span),
    )
    sums = (sums_ref[...] + 1e-06, other_sums_ref[...] + 1e-06)
    weight = [weight_sq_ref[:, c] + 1e-06 for c in columns]
    total = sum(jnp.sum(jnp.sqrt(s / w), 1, keepdims=True) for s, w in zip(sums, weight))
    mean_ratio = total / width
    fans = (first_ref.shape[0] * wide, second_ref.shape[0] * wide)
    for c, s, w, value_ref in zip(columns, sums, weight, (own_ref, other_ref)):
        factor = jnp.minimum(1.0 / (mean_ratio * jnp.sqrt(w)), 1.0 / jnp.sqrt(s))
        value = value_ref[share]
        first_ref[:, c] = value[:first_rows] * (factor[0:1] * math.sqrt(fans[0]))
        second_ref[:, c] = value[first_rows:] * (factor[1:2] * math.sqrt(fans[1]))


def swap_pairs(size, mask):
    return [(i, i ^ mask) for i in range(size)]


def crossed(value, even_mask, odd_mask):
    wide, narrow = lax.axis_size("wide"), lax.axis_size("narrow")
    pairs = []
    for i in range(wide):
        for j in range(narrow):
            pairs.append((i * narrow + j, (i ^ (odd_mask if j % 2 else even_mask)) * narrow + j))
    return lax.ppermute(value, ("wide", "narrow"), pairs)


def device_step(
    node_latent,
    edge_latent,
    node_cotangent,
    w_first,
    bias_first,
    w_second,
    bias_second,
    norm_gain,
    send_map,
    edge_sender,
    edge_receiver,
):
    nodes, width = node_latent.shape
    edges = edge_latent.shape[0]
    slots = send_map.shape[2]
    wide, narrow = lax.axis_size("wide"), lax.axis_size("narrow")
    if wide < 4 or wide & (wide - 1) or narrow < 2 or narrow & (narrow - 1):
        raise ValueError("axis sizes")
    routes = routes_of()
    blocks = len(routes)
    table_rows = nodes + blocks * slots

    def like(shape, kind):
        return jax.ShapeDtypeStruct(shape, kind)

    halo = [like((slots, width), BF)] * blocks
    send_slots, node, *outgoing = local_call(
        gather_body,
        [like(send_map.shape, jnp.int32), like((nodes, width), BF), *halo],
        (send_map, node_latent),
        0.1,
        far=2,
        scratch=[pltpu.SemaphoreType.DMA((2,))],
    )
    received = []
    for block, (axis, (pairs, _, _)) in zip(outgoing, routes):
        received.append(lax.ppermute(block, axis, pairs))
    start, sender_hot, receiver_hot, edge_t, up, weight_sq, cot, weights, weights_2, weights_2t, near_rows, far_rows, vectors = local_call(
        functools.partial(prepare_body, slots=slots),
        [
            like((edges, width), F32),
            like((table_rows, edges), BF),
            like((nodes, edges), BF),
            like((width, edges), BF),
            like((edges, width), BF),
            like((2, width), F32),
            like((nodes, width), BF),
            like(w_first.shape, BF),
            like(w_second.shape, BF),
            like(w_second.shape[::-1], BF),
            like((edges, table_rows - 2 * slots), BF),
            like((edges, 4 * slots), BF),
            like((2, width), F32),
        ],
        (
            edge_sender.reshape(1, edges),
            edge_receiver.reshape(1, edges),
            node_cotangent,
            edge_latent,
            w_first,
            w_second,
            bias_first,
            bias_second,
            norm_gain,
            node,
        ),
        1.0,
        far=9,
        scratch=[
            pltpu.VMEM((1, edges), jnp.int32),
            pltpu.VMEM((1, edges), jnp.int32),
            pltpu.VMEM((edges, width), BF),
            *[pltpu.VMEM((width,), BF)] * 3,
            pltpu.SemaphoreType.DMA((9,)),
        ],
    )
    start, scaled = local_call(
        near_body,
        [like((edges, width), F32), like((edges, width), F32)],
        (start, near_rows, up, node, weights, vectors, *received[2:]),
        0.5,
    )
    pre_back, norm_back, act_t = local_call(
        middle_body,
        [like((edges, width), BF), like((edges, width), BF), like((width, edges), BF)],
        (start, far_rows, scaled, *received[:2], weights, weights_2, weights_2t, vectors),
        1.0,
    )
    first_rows, second_rows = w_first.shape[0] // wide, w_second.shape[0] // wide
    rows = first_rows + second_rows
    span = width // 2
    heights = [end - begin for begin, end in chain_cuts(rows)]
    operands = (edge_t, act_t, sender_hot, receiver_hot, pre_back, norm_back, node, *received)

    def outer(own, kind):
        return local_call(
            functools.partial(outer_body, blocks=blocks, own=own),
            [like((wide, height, span), kind) for height in heights],
            operands,
            0.6,
        )

    half_swap = swap_pairs(narrow, narrow // 2)
    gots = [lax.ppermute(sent, "narrow", half_swap) for sent in outer(False, BF)]
    kepts = list(outer(True, F32))
    edge_grad, own_grad, *halo_grad = local_call(
        functools.partial(back_body, blocks=blocks, slots=slots),
        [like((edges, width), BF), like((nodes, width), F32), *halo],
        (pre_back, weights, up, cot, sender_hot, receiver_hot),
        1.0,
    )
    mask = narrow // 4
    while mask:
        span //= 2
        bit = (lax.axis_index("narrow") // mask) % 2
        for c in range(CHAINS):
            value = kepts[c] + gots[c].astype(F32)
            sent = lax.dynamic_slice_in_dim(value, (1 - bit) * span, span, 2).astype(BF)
            kepts[c] = lax.dynamic_slice_in_dim(value, bit * span, span, 2)
            gots[c] = lax.ppermute(sent, "narrow", swap_pairs(narrow, mask))
        mask //= 2
    bits = wide.bit_length() - 1
    for step in range(bits - 1):
        masks = [(1, 2), (2, 1)][step] if step < 2 else (1 << step, 1 << step)
        for c in range(CHAINS):
            shape = (wide >> (step + 1), heights[c], span)
            kepts[c], sent = local_call(
                functools.partial(combine_body, step=step),
                [like(shape, F32), like(shape, BF)],
                (kepts[c], gots[c]),
                0.01,
            )
            gots[c] = crossed(sent, *masks)
    top = wide // 2
    for c in range(CHAINS):
        shape = (2, heights[c], span)
        kepts[c], sent = local_call(
            whole_body, [like(shape, F32), like(shape, BF)], (kepts[c], gots[c]), 0.01
        )
        gots[c] = crossed(sent, top, top)
        if narrow > 2:
            (value,) = local_call(finish_body, [like(shape, F32)], (kepts[c], gots[c]), 0.01)
            mask = 1
            while mask < narrow // 2:
                other = lax.ppermute(value, "narrow", swap_pairs(narrow, mask))
                value = jnp.where(
                    (lax.axis_index("narrow") // mask) % 2 == 0,
                    jnp.concatenate([value, other], 2),
                    jnp.concatenate([other, value], 2),
                )
                mask *= 2
            kepts[c], gots[c] = value, jnp.zeros(value.shape, BF)
    returned = []
    for block, (axis, (pairs, _, _)) in zip(halo_grad, routes):
        returned.append(lax.ppermute(block, axis, [(t, s) for s, t in pairs]))
    (node_grad,) = local_call(
        return_body, [like((nodes, width), BF)], (send_slots, own_grad, *returned), 0.1
    )
    value, sums = local_call(
        functools.partial(sums_body, first_rows=first_rows),
        [like((2, rows, width // 2), F32), like((2, width // 2), F32)],
        (*kepts, *gots),
        0.001,
    )
    other = lax.ppermute(value, "narrow", half_swap)
    for position in range(bits - 1):
        arrived = lax.ppermute(sums, "wide", swap_pairs(wide, 1 << position))
        sums = sums + arrived
    other_sums = lax.ppermute(sums, "narrow", half_swap)
    first_update, second_update = local_call(
        functools.partial(clip_body, top=top),
        [like((first_rows, width), F32), like((second_rows, width), F32)],
        (value, other, sums, other_sums, weight_sq),
        0.001,
    )
    return (node_grad, edge_grad, first_update, second_update)


def solution(mesh):
    return jax.shard_map(
        device_step,
        mesh=mesh,
        in_specs=(
            P(("wide", "narrow"), None),
            P(("wide", "narrow"), None),
            P(("wide", "narrow"), None),
            P(),
            P(),
            P(),
            P(),
            P(),
            P(("wide", "narrow"), None, None),
            P(("wide", "narrow")),
            P(("wide", "narrow")),
        ),
        out_specs=(
            P(("wide", "narrow"), None),
            P(("wide", "narrow"), None),
            P("wide", None),
            P("wide", None),
        ),
        check_vma=False,
    )
```
